32 devices in a mesh: dp: 1 (over z), ep: 32 (over y, x, core).
Axes of the slice: x: 4, y: 4, z: 1, core: 2. Of those that a mesh axis runs over, the one named last changes fastest.
The devices are a block of a 4x4x8 slice.
Arguments:
- x: bfloat16 [24576, 2048], P(('dp', 'ep'))
- route_idx: int32 [24576, 2], P(('dp', 'ep'))
- gates: float32 [24576, 2], P(('dp', 'ep'))
- w1: bfloat16 [32, 2048, 1408], P('ep')
- w3: bfloat16 [32, 2048, 1408], P('ep')
- w2: bfloat16 [32, 1408, 2048], P('ep')
Outputs:
- output: bfloat16 [24576, 2048], P(('dp', 'ep'))
All inputs are finite; a program needn't handle non-finite values.
Results may differ from the reference program's by a relative error of at most 0.00125.
Values are sent between devices in bfloat16 or wider.
A program may use at most 768 MiB of HBM per device.

```python
import jax
import jax.numpy as jnp
from jax import lax

D = 2048
FF = 1408
TOK = 768
EP = 32

T = EP * TOK
RB = TOK // 2
NB = 2 * T // RB + EP


def build_route(counts, key):
    ks, kp = jax.random.split(key)
    cum = jnp.cumsum(counts, axis=1)
    r = jnp.arange(TOK)
    s0 = jax.vmap(lambda c: jnp.searchsorted(c, r, side='right'))(cum)
    s1 = jnp.roll(s0, -(TOK // 2), axis=1)
    pairs = jnp.stack([s0, s1], axis=-1).astype(jnp.int32)
    swap = jax.random.bernoulli(ks, 0.5, (EP, TOK))
    pairs = jnp.where(swap[:, :, None], pairs[:, :, ::-1], pairs)
    keys = jax.random.split(kp, EP)
    pairs = jax.vmap(lambda k, p: jax.random.permutation(k, p, axis=0))(keys, pairs)
    return pairs.reshape(T, 2)


def setup_inputs(seed: int = 0, part: int = 0) -> dict:
    key = jax.random.fold_in(jax.random.key(seed), part)
    kx, kr, kg, kh, kc = jax.random.split(key, 5)
    kw1, kw3, kw2 = jax.random.split(jax.random.key(seed + 1), 3)
    x = jax.random.normal(kx, (T, D), jnp.float32).astype(jnp.bfloat16)
    dev = jnp.arange(EP)
    perm = jax.random.permutation(kh, EP)
    hot = perm[:3]
    cold = perm[3:]
    extra = jax.random.randint(kc, (EP, TOK // 4 - EP + 3), 0, EP - 3)
    cold_cnt = jnp.ones((EP, EP - 3), jnp.int32).at[dev[:, None], extra].add(1)
    counts = jnp.zeros((EP, EP), jnp.int32).at[:, cold].set(cold_cnt)
    amt = jnp.array([3 * TOK // 8, TOK // 4, TOK // 8], jnp.int32)
    hot_idx = hot[(jnp.arange(3)[None, :] + dev[:, None]) % 3]
    counts = counts.at[dev[:, None], hot_idx].set(jnp.broadcast_to(amt, (EP, 3)))
    route_idx = build_route(counts, kr)
    g0 = jax.random.uniform(kg, (T,), jnp.float32, 0.3, 0.7)
    gates = jnp.stack([g0, 1.0 - g0], axis=1)
    w1 = (jax.random.normal(kw1, (EP, D, FF), jnp.float32) * D ** -0.5).astype(jnp.bfloat16)
    w3 = (jax.random.normal(kw3, (EP, D, FF), jnp.float32) * D ** -0.5).astype(jnp.bfloat16)
    w2 = (jax.random.normal(kw2, (EP, FF, D), jnp.float32) * FF ** -0.5).astype(jnp.bfloat16)
    return {'x': x, 'route_idx': route_idx, 'gates': gates, 'w1': w1, 'w3': w3, 'w2': w2}


def reference(x, route_idx, gates, w1, w3, w2):
    e = route_idx.reshape(-1)
    g = gates.reshape(-1)
    tk = jnp.arange(2 * T, dtype=jnp.int32) // 2
    order = jnp.argsort(e, stable=True)
    se = e[order]
    counts = jnp.zeros((EP,), jnp.int32).at[e].add(1)
    start = jnp.cumsum(counts) - counts
    padded = (counts + RB - 1) // RB * RB
    pend = jnp.cumsum(padded)
    pstart = pend - padded
    dest = pstart[se] + jnp.arange(2 * T, dtype=jnp.int32) - start[se]
    tbuf = jnp.full((NB * RB,), T, jnp.int32).at[dest].set(tk[order])
    gbufv = jnp.zeros((NB * RB,), jnp.float32).at[dest].set(g[order])
    bexp = jnp.minimum(jnp.searchsorted(pend, jnp.arange(NB) * RB, side='right'), EP - 1)
    xe = jnp.concatenate([x, jnp.zeros((1, D), x.dtype)], axis=0)

    def step(y, blk):
        tb, gb, be = blk
        rows = xe[tb]
        a = jnp.dot(rows, w1[be], preferred_element_type=jnp.float32)
        b = jnp.dot(rows, w3[be], preferred_element_type=jnp.float32)
        h = (jax.nn.silu(a) * b).astype(jnp.bfloat16)
        o = jnp.dot(h, w2[be], preferred_element_type=jnp.float32).astype(jnp.bfloat16)
        return y.at[tb].add(gb[:, None] * o.astype(jnp.float32)), None

    y, _ = lax.scan(step, jnp.zeros((T + 1, D), jnp.float32),
                    (tbuf.reshape(NB, RB), gbufv.reshape(NB, RB), bexp))
    return y[:T].astype(jnp.bfloat16)
```

```python
import jax
import jax.numpy as jnp
from jax import lax
from jax.sharding import PartitionSpec as P

CAP = 40
ROUND_COST = 200
HOT_COST = 100


def pair_slots(oh):
    n = oh.shape[0]
    i = jnp.arange(n, dtype=jnp.int32)
    low = (i[None, :] < i[:, None]).astype(jnp.bfloat16)
    before = jnp.dot(low, jnp.sum(oh, axis=1).astype(jnp.bfloat16), preferred_element_type=jnp.float32)
    return jnp.sum(before[:, None, :] * oh, axis=2).astype(jnp.int32)


def plan(most):
    ne = most.shape[0]
    i = jnp.arange(ne, dtype=jnp.int32)
    ahead = (most[None, :] > most[:, None]) | ((most[None, :] == most[:, None]) & (i[None, :] < i[:, None]))
    rank = jnp.sum(ahead.astype(jnp.int32), axis=1)
    k = jnp.arange(ne + 1, dtype=jnp.int32)
    left = jnp.max(jnp.where(rank[None, :] >= k[:, None], most[None, :], 0), axis=1)
    cost = k * HOT_COST + (left + CAP - 1) // CAP * ROUND_COST
    nhot = jnp.argmin(cost).astype(jnp.int32)
    rounds = jnp.sum(jnp.where(k == nhot, (left + CAP - 1) // CAP, 0))
    order = jnp.sum(jnp.where(rank[None, :] == i[:, None], i[None, :], 0), axis=1)
    return rank, order, nhot, rounds


def experts(rows, w1, w3, w2):
    a = jnp.dot(rows, w1, preferred_element_type=jnp.float32)
    b = jnp.dot(rows, w3, preferred_element_type=jnp.float32)
    h = (jax.nn.silu(a) * b).astype(jnp.bfloat16)
    return jnp.dot(h, w2, preferred_element_type=jnp.float32).astype(jnp.bfloat16)


def take(x, dest, nrows):
    r = jnp.arange(nrows, dtype=dest.dtype)[:, None]
    p = (dest[None, :, 0] == r) | (dest[None, :, 1] == r)
    return jnp.dot(p.astype(x.dtype), x)


def put(back, dest, gates):
    r = jnp.arange(back.shape[0], dtype=dest.dtype)[None, :]
    o0 = jnp.dot((dest[:, 0:1] == r).astype(back.dtype), back, preferred_element_type=jnp.float32)
    o1 = jnp.dot((dest[:, 1:2] == r).astype(back.dtype), back, preferred_element_type=jnp.float32)
    return gates[:, 0:1] * o0 + gates[:, 1:2] * o1


def solution(mesh):
    ep = mesh.shape['ep']

    def local(x, route_idx, gates, w1, w3, w2):
        tok, d = x.shape
        w1, w3, w2 = w1[0], w3[0], w2[0]
        me = lax.axis_index('ep')
        oh = (route_idx[:, :, None] == jnp.arange(ep, dtype=route_idx.dtype)).astype(jnp.float32)
        pos = pair_slots(oh)
        most = lax.pmax(jnp.sum(oh, axis=(0, 1)).astype(jnp.int32), 'ep')
        rank, order, nhot, rounds = plan(most)
        rk = jnp.sum(oh * rank.astype(jnp.float32), axis=2).astype(jnp.int32)
        cold = rk >= nhot

        def one_round(r, y):
            here = cold & (pos // CAP == r)
            dest = jnp.where(here, route_idx * CAP + pos - r * CAP, -1)
            send = take(x, dest, ep * CAP).reshape(ep, CAP, d)
            recv = lax.all_to_all(send, 'ep', 0, 0, tiled=True).reshape(ep * CAP, d)
            out = experts(recv, w1, w3, w2).reshape(ep, CAP, d)
            back = lax.all_to_all(out, 'ep', 0, 0, tiled=True).reshape(ep * CAP, d)
            return y + put(back, dest, gates)

        def one_hot(j, y):
            e = jnp.sum(jnp.where(jnp.arange(ep) == j, order, 0))
            mine = me == e
            v1, v3, v2 = lax.psum(tuple(jnp.where(mine, w, jnp.zeros_like(w)) for w in (w1, w3, w2)), 'ep')
            n = 3 * tok // 4
            dest = jnp.where(rk == j, pos, -1)
            out = experts(take(x, dest, n), v1, v3, v2)
            return y + put(out, dest, gates)

        y = jnp.zeros((tok, d), jnp.float32)
        y = lax.fori_loop(0, rounds, one_round, y)
        y = lax.fori_loop(0, nhot, one_hot, y)
        return y.astype(jnp.bfloat16)

    spec = P(('dp', 'ep'), None)
    wspec = P('ep', None, None)
    return jax.shard_map(local, mesh=mesh, in_specs=(spec, spec, spec, wspec, wspec, wspec),
                         out_specs=spec, check_vma=False)
```

```python
import functools
import math

import jax
import jax.numpy as jnp
from jax import lax
from jax.experimental import pallas as pl
from jax.experimental.pallas import tpu as pltpu
from jax.sharding import PartitionSpec as P

MESH = pl.DeviceIdType.MESH
CAP = 40
SLOTS = 3
ROWS = 16
LAG = 4
TM = 192


@functools.lru_cache(None)
def rings(n):
    def near(v):
        y, x = divmod(v, n)
        return [y * n + (x + 1) % n, y * n + (x - 1) % n, (y + 1) % n * n + x, (y - 1) % n * n + x]

    def edges(c):
        return {frozenset((c[i], c[(i + 1) % len(c)])) for i in range(len(c))}

    def cycle(used):
        v, c = 0, [0]
        prev = None
        while True:
            step = [w for w in near(v) if frozenset((v, w)) not in used and w != prev]
            prev, v = v, step[0]
            if v == 0 or v in c:
                return c
            c.append(v)

    def search(path, seen):
        if len(path) == n * n:
            if path[0] in near(path[-1]):
                other = cycle(edges(path))
                if len(other) == n * n and not edges(other) & edges(path):
                    return list(path), other
            return None
        for w in near(path[-1]):
            if w not in seen:
                found = search(path + [w], seen | {w})
                if found:
                    return found
        return None

    a, b = search([0], {0})
    nxt, pos = [], []
    for c in (a, a[::-1], b, b[::-1]):
        nx, ps = [0] * len(c), [0] * len(c)
        for i, v in enumerate(c):
            nx[v], ps[v] = c[(i + 1) % len(c)], i
        nxt.append(nx)
        pos.append(ps)
    return nxt, pos


def counts_kernel(ep, c_ref, out_ref, send_sem, recv_sem):
    me = lax.axis_index('ep')
    out_ref[me] = c_ref[...]

    def send(i, _):
        pltpu.make_async_remote_copy(
            src_ref=c_ref, dst_ref=out_ref.at[me], send_sem=send_sem, recv_sem=recv_sem,
            device_id={'ep': lax.rem(me + i, ep)}, device_id_type=MESH).start()
        return 0

    lax.fori_loop(1, ep, send, 0)
    others = out_ref.at[pl.ds(0, ep - 1)]
    pltpu.make_async_copy(others, others, send_sem).wait()
    pltpu.make_async_copy(others, others, recv_sem).wait()


def gather_counts(c, ep):
    return pl.pallas_call(
        functools.partial(counts_kernel, ep),
        name='gather_counts',
        out_shape=jax.ShapeDtypeStruct((ep,) + c.shape, c.dtype),
        in_specs=[pl.BlockSpec(memory_space=pltpu.VMEM)],
        out_specs=pl.BlockSpec(memory_space=pltpu.VMEM),
        scratch_shapes=[pltpu.SemaphoreType.DMA, pltpu.SemaphoreType.DMA],
        compiler_params=pltpu.CompilerParams(has_side_effects=True),
    )(c)


def ring_kernel(nxt, steps, mask_ref, w1_ref, w3_ref, w2_ref, out_ref, sib_ref, recv, inj,
                s_next, s_sib, s_out, r_next, r_sib, sib_send, sib_recv, inj_sem):
    chips = len(nxt[0])
    own = (w1_ref, w3_ref, w2_ref)
    per = w1_ref.shape[2]
    chunks = len(own) * per
    me = lax.axis_index('ep')
    chip, core = me // 2, me % 2
    sib = me + 1 - 2 * core
    to = []
    for r in range(4):
        t = jnp.int32(0)
        for i in range(chips):
            t = jnp.where(chip == i, nxt[r][i], t)
        to.append(t * 2 + core)
    chains = [(j, r) for j in range(SLOTS) for r in range(4)]

    def push(q):
        return pltpu.make_async_remote_copy(
            src_ref=own[q].at[1 - core], dst_ref=sib_ref.at[q], send_sem=sib_send.at[q],
            recv_sem=sib_recv.at[q], device_id={'ep': sib}, device_id_type=MESH)

    for q in range(len(own)):
        push(q).start()

    def loads(q, t):
        k = lax.rem(t, LAG)
        return (pltpu.make_async_copy(own[q].at[core, :, lax.rem(t, per)], inj.at[k, 0], inj_sem.at[k, 0]),
                pltpu.make_async_copy(sib_ref.at[q, :, lax.rem(t, per)], inj.at[k, 1], inj_sem.at[k, 1]))

    def fetch(t):
        for q in range(len(own)):
            @pl.when(t == q * per)
            def _():
                push(q).wait_recv()

            @pl.when(t // per == q)
            def _():
                for c in loads(q, t):
                    c.start()

    def hop(t, j, r):
        pltpu.make_async_remote_copy(
            src_ref=recv.at[t, j, r], dst_ref=recv.at[t + 1, j, r], send_sem=s_next.at[lax.rem(t, LAG)],
            recv_sem=r_next.at[lax.rem(t + 1, chips), j, r], device_id={'ep': to[r]}, device_id_type=MESH).start()

    def keep(t):
        pltpu.make_async_remote_copy(
            src_ref=recv.at[t], dst_ref=out_ref.at[core, t], send_sem=s_sib.at[lax.rem(t, LAG)],
            recv_sem=r_sib.at[t], device_id={'ep': sib}, device_id_type=MESH).start()
        pltpu.make_async_copy(recv.at[t], out_ref.at[core, t], s_out.at[lax.rem(t, LAG)]).start()

    def drain(t, last):
        whole = recv.at[t]
        for s in (s_sib, s_out) if last else (s_next, s_sib, s_out):
            pltpu.make_async_copy(whole, whole, s.at[lax.rem(t, LAG)]).wait()

    def arrive(t, j, r):
        here = recv.at[t, j, r]
        pltpu.make_async_copy(here, here, r_next.at[lax.rem(t, chips), j, r]).wait()

    def step(t, first, inject, last):
        if inject:
            for c in loads(0, t):
                c.wait()
            k = lax.rem(t, LAG)

            @pl.when(t + LAG - 1 < chunks)
            def _():
                fetch(t + LAG - 1)

        @pl.when(t >= LAG - 1)
        def _():
            drain(t - (LAG - 1), False)

        before = None
        for j, r in chains:
            if not first:
                arrive(t, j, r)
            if inject:
                mine, theirs = mask_ref[j, 0] > 0, mask_ref[j, 1] > 0
                for c in range(recv.shape[-1] // 128):
                    cols = pl.ds(c * 128, 128)
                    other = inj[k, 1, r, :, cols]
                    old = other if first else recv[t, j, r, :, cols]
                    recv[t, j, r, :, cols] = jnp.where(mine, inj[k, 0, r, :, cols], jnp.where(theirs, other, old))
            if before is not None and not last:
                hop(t, *before)
            before = (j, r)
        if not last:
            hop(t, *before)
        keep(t)

    for t in range(LAG - 1):
        fetch(jnp.int32(t))
    step(jnp.int32(0), True, True, False)
    lax.fori_loop(1, chunks, lambda t, c: (step(t, False, True, False), c)[1], 0)
    lax.fori_loop(chunks, steps - 1, lambda t, c: (step(t, False, False, False), c)[1], 0)
    step(jnp.int32(steps - 1), False, False, True)
    for t in range(steps - LAG + 1, steps):
        drain(jnp.int32(t), t == steps - 1)

    def settle(t, c):
        part = out_ref.at[1 - core, t]
        pltpu.make_async_copy(part, part, r_sib.at[t]).wait()
        return c

    lax.fori_loop(0, steps, settle, 0)
    for q in range(len(own)):
        push(q).wait_send()


def broadcast(masks, w1, w3, w2t, nxt):
    _, nr, per, rows, cols = w1.shape
    steps = 3 * per + len(nxt[0]) - 1
    dma = pltpu.SemaphoreType.DMA
    hbm = pl.BlockSpec(memory_space=pl.ANY)
    out, _ = pl.pallas_call(
        functools.partial(ring_kernel, nxt, steps),
        name='ring_broadcast',
        out_shape=(jax.ShapeDtypeStruct((2, steps, SLOTS, nr, rows, cols), w1.dtype),
                   jax.ShapeDtypeStruct((3, nr, per, rows, cols), w1.dtype)),
        in_specs=[pl.BlockSpec(memory_space=pltpu.VMEM), hbm, hbm, hbm],
        out_specs=(hbm, hbm),
        scratch_shapes=[
            pltpu.VMEM((steps, SLOTS, nr, rows, cols), w1.dtype),
            pltpu.VMEM((LAG, 2, nr, rows, cols), w1.dtype),
            dma((LAG,)), dma((LAG,)), dma((LAG,)), dma((len(nxt[0]), SLOTS, nr)), dma((steps,)),
            dma((3,)), dma((3,)), dma((LAG, 2)),
        ],
        compiler_params=pltpu.CompilerParams(has_side_effects=True, vmem_limit_bytes=60 * 1024 * 1024),
    )(masks, w1, w3, w2t)
    return out


def hot_kernel(info_ref, x_ref, drow_ref, dcol_ref, gcol_ref, got_ref, y0_ref, y_ref,
               w, a, b, h, xg, p2, w_sem, y_sem):
    tok, d = x_ref.shape
    nr = got_ref.shape[3]
    per = w.shape[3]
    f = got_ref.shape[5]
    blk = per * ROWS

    def loads(j, start):
        for q in range(3):
            for c in range(2):
                for r in range(nr):
                    cp = pltpu.make_async_copy(
                        got_ref.at[c, pl.ds(info_ref[j, 1 + r] + q * per, per), j, r],
                        w.at[j % 2, q, c * nr + r], w_sem.at[j % 2, q, c * nr + r])
                    cp.start() if start else cp.wait()

    loads(0, True)
    fill = pltpu.make_async_copy(y0_ref, y_ref, y_sem)
    fill.start()
    fill.wait()
    for j in range(SLOTS):
        if j + 1 < SLOTS:
            loads(j + 1, True)
        loads(j, False)

        def tile(m, carry, j=j):
            base = m * TM
            p = (drow_ref[j:j + 1, :] == base + lax.broadcasted_iota(jnp.int32, (TM, tok), 0)).astype(jnp.bfloat16)
            p2[...] = (dcol_ref[:, j:j + 1] == base + lax.broadcasted_iota(jnp.int32, (tok, TM), 1)).astype(jnp.bfloat16)

            def up(i, c):
                cols = pl.ds(pl.multiple_of(i * blk, blk), blk)
                xs = jnp.dot(p, x_ref[:, cols], preferred_element_type=jnp.float32).astype(jnp.bfloat16)
                da = jnp.dot(xs, w[j % 2, 0, i].reshape(blk, f), preferred_element_type=jnp.float32)
                db = jnp.dot(xs, w[j % 2, 1, i].reshape(blk, f), preferred_element_type=jnp.float32)

                @pl.when(i == 0)
                def _():
                    a[...] = da
                    b[...] = db

                @pl.when(i > 0)
                def _():
                    a[...] += da
                    b[...] += db
                return c

            lax.fori_loop(0, 2 * nr, up, 0)
            h[...] = (jax.nn.silu(a[...]) * b[...]).astype(jnp.bfloat16)

            def down(i, c):
                cols = pl.ds(pl.multiple_of(i * blk, blk), blk)
                o = lax.dot_general(h[...], w[j % 2, 2, i].reshape(blk, f), (((1,), (1,)), ((), ())),
                                    preferred_element_type=jnp.float32).astype(jnp.bfloat16)
                y_ref[:, cols] += gcol_ref[:, j:j + 1] * jnp.dot(p2[...], o, preferred_element_type=jnp.float32)
                return c

            lax.fori_loop(0, 2 * nr, down, 0)
            return carry

        lax.fori_loop(0, (info_ref[j, 0] + TM - 1) // TM, tile, 0)


def hot_rows(info, x, drow, dcol, gcol, got, y0):
    tok, d = x.shape
    _, _, _, nr, rows, f = got.shape
    per = d // (2 * nr * rows)
    vmem, hbm = pl.BlockSpec(memory_space=pltpu.VMEM), pl.BlockSpec(memory_space=pl.ANY)
    return pl.pallas_call(
        hot_kernel,
        name='hot_rows',
        out_shape=jax.ShapeDtypeStruct(y0.shape, y0.dtype),
        in_specs=[pl.BlockSpec(memory_space=pltpu.SMEM), vmem, vmem, vmem, vmem, hbm, hbm],
        out_specs=vmem,
        scratch_shapes=[
            pltpu.VMEM((2, 3, 2 * nr, per, rows, f), x.dtype),
            pltpu.VMEM((TM, f), jnp.float32), pltpu.VMEM((TM, f), jnp.float32), pltpu.VMEM((TM, f), x.dtype),
            pltpu.VMEM((8, 128), x.dtype), pltpu.VMEM((tok, TM), x.dtype),
            pltpu.SemaphoreType.DMA((2, 3, 2 * nr)), pltpu.SemaphoreType.DMA,
        ],
        compiler_params=pltpu.CompilerParams(vmem_limit_bytes=60 * 1024 * 1024),
    )(info, x, drow, dcol, gcol, got, y0)


def pair_slots(oh):
    n = oh.shape[0]
    i = jnp.arange(n, dtype=jnp.int32)
    low = (i[None, :] < i[:, None]).astype(jnp.bfloat16)
    before = jnp.dot(low, jnp.sum(oh, axis=1).astype(jnp.bfloat16), preferred_element_type=jnp.float32)
    return jnp.sum(before[:, None, :] * oh, axis=2).astype(jnp.int32)


def plan(most, worst):
    ne = most.shape[0]
    i = jnp.arange(ne, dtype=jnp.int32)
    ahead = (most[None, :] > most[:, None]) | ((most[None, :] == most[:, None]) & (i[None, :] < i[:, None]))
    rank = jnp.sum(ahead.astype(jnp.int32), axis=1)
    k = jnp.arange(ne + 1, dtype=jnp.int32)
    left = worst(jnp.max(jnp.where(rank[None, :] >= k[:, None], most[None, :], 0), axis=1))
    hot_cost = (k + SLOTS - 1) // SLOTS * 260 + k
    cost = hot_cost + (left + CAP - 1) // CAP * 170
    nhot = jnp.argmin(cost).astype(jnp.int32)
    rounds = jnp.sum(jnp.where(k == nhot, (left + CAP - 1) // CAP, 0))
    order = jnp.sum(jnp.where(rank[None, :] == i[:, None], i[None, :], 0), axis=1)
    return rank, order, nhot, rounds


def experts(rows, w1, w3, w2):
    a = jnp.dot(rows, w1, preferred_element_type=jnp.float32)
    b = jnp.dot(rows, w3, preferred_element_type=jnp.float32)
    h = (jax.nn.silu(a) * b).astype(jnp.bfloat16)
    return jnp.dot(h, w2, preferred_element_type=jnp.float32).astype(jnp.bfloat16)


def take(x, dest, nrows):
    r = jnp.arange(nrows, dtype=dest.dtype)[:, None]
    p = (dest[None, :, 0] == r) | (dest[None, :, 1] == r)
    return jnp.dot(p.astype(x.dtype), x)


def put(back, dest, gates):
    r = jnp.arange(back.shape[0], dtype=dest.dtype)[None, :]
    o0 = jnp.dot((dest[:, 0:1] == r).astype(back.dtype), back, preferred_element_type=jnp.float32)
    o1 = jnp.dot((dest[:, 1:2] == r).astype(back.dtype), back, preferred_element_type=jnp.float32)
    return gates[:, 0:1] * o0 + gates[:, 1:2] * o1


def solution(mesh):
    ep = mesh.shape['ep']
    groups = mesh.shape['dp']
    nxt, pos_of = rings(math.isqrt(ep // 2))

    def local(x, route_idx, gates, w1, w3, w2):
        tok, d = x.shape
        w1, w3, w2 = w1[0], w3[0], w2[0]
        f = w1.shape[1]
        w2t = w2.T
        me = lax.axis_index('ep')
        i = jnp.arange(ep, dtype=jnp.int32)
        oh = (route_idx[:, :, None] == i).astype(jnp.float32)
        pos = pair_slots(oh)
        mine = jnp.sum(oh, axis=(0, 1))
        table = gather_counts(jnp.zeros((8, 128), jnp.float32).at[0, :ep].set(mine), ep)
        most = jnp.max(table[:, 0, :ep], axis=0).astype(jnp.int32)
        worst = (lambda v: lax.pmax(v, 'dp')) if groups > 1 else (lambda v: v)
        rank, order, nhot, rounds = plan(most, worst)
        rk = jnp.sum(oh * rank.astype(jnp.float32), axis=2).astype(jnp.int32)
        cold = rk >= nhot

        def one_round(r, y):
            here = cold & (pos // CAP == r)
            dest = jnp.where(here, route_idx * CAP + pos - r * CAP, -1)
            send = take(x, dest, ep * CAP).reshape(ep, CAP, d)
            recv = lax.all_to_all(send, 'ep', 0, 0, tiled=True).reshape(ep * CAP, d)
            out = experts(recv, w1, w3, w2).reshape(ep, CAP, d)
            back = lax.all_to_all(out, 'ep', 0, 0, tiled=True).reshape(ep * CAP, d)
            return y + put(back, dest, gates)

        def some_hot(it, y):
            shape = (2, 4, -1, ROWS, f)
            slot = it * SLOTS + jnp.arange(SLOTS, dtype=jnp.int32)
            src = jnp.sum(jnp.where(i[None, :] == slot[:, None], order[None, :], 0), axis=1)
            flags = jnp.stack([src == me, src == me + 1 - 2 * (me % 2)], axis=1)
            masks = jnp.broadcast_to(flags[:, :, None, None], (SLOTS, 2, ROWS, 128)).astype(jnp.bfloat16)
            got = broadcast(masks, w1.reshape(shape), w3.reshape(shape), w2t.reshape(shape), nxt)
            place = jnp.array(pos_of, jnp.int32)
            chip = jnp.arange(ep // 2, dtype=jnp.int32)
            at = jnp.sum(jnp.where(chip == me // 2, place, 0), axis=1)[None, :]
            at = at - jnp.sum(jnp.where((chip[None, :] == src[:, None] // 2)[:, None, :], place[None], 0), axis=2)
            at = jnp.where(at < 0, at + ep // 2, at)
            match = (rk[:, :, None] == slot) & (rk < nhot)[:, :, None]
            dcol = jnp.sum(jnp.where(match, pos[:, :, None] + 1, 0), axis=1) - 1
            gcol = jnp.sum(jnp.where(match, gates[:, :, None], 0), axis=1)
            cnt = jnp.sum((dcol >= 0).astype(jnp.int32), axis=0)
            info = jnp.concatenate([cnt[:, None], at], axis=1)
            return hot_rows(info, x, dcol.T, dcol, gcol, got, y)

        y = jnp.zeros((tok, d), jnp.float32)
        y = lax.fori_loop(0, rounds, one_round, y)
        y = lax.fori_loop(0, (nhot + SLOTS - 1) // SLOTS, some_hot, y)
        return y.astype(jnp.bfloat16)

    spec = P(('dp', 'ep'), None)
    wspec = P('ep', None, None)
    return jax.shard_map(local, mesh=mesh, in_specs=(spec, spec, spec, wspec, wspec, wspec),
                         out_specs=spec, check_vma=False)
```
